32 devices in a mesh: section: 8 (over z, y), fsdp: 4 (over x, core).
Axes of the slice: x: 2, y: 2, z: 4, core: 2. Of those that a mesh axis runs over, the one named last changes fastest.
Arguments:
- source_rows: bfloat16 [3072, 4096], P(('section', 'fsdp')), may hold values from -6 to 6
- target_rows: bfloat16 [1024, 4096], P('section'), may hold values from -6 to 6
- attn_weights: bfloat16 [8, 4, 4096, 3072], P('section', None, None, 'fsdp'), may hold values from -3.76875 to 3.76875
- gains: float32 [8, 4096], P('section'), may hold values from 0.25 to 1.75
- lengths: int32 [8], P('section'), may hold values from 192 to 384
Outputs:
- source_next: bfloat16 [3072, 4096], P(('section', 'fsdp'))
- target_next: bfloat16 [1024, 4096], P('section')
The draws below stay inside these ranges and needn't reach their ends.
Inputs may be any that keep to these rules, and one draw needn't show every extreme that they name: Keys at positions lengths[s] and beyond are padding.
All inputs are finite; a program needn't handle non-finite values.
Results may differ from the reference program's by a relative error of at most 0.015.
The reference program's roundings to bfloat16 on the way count: a program that leaves them out, or rounds other values in their place, can miss the bound.
Values may be sent and summed in bfloat16 or wider, within the bound.
A program may use at most 128 MiB of HBM per device.

```python
import math
import jax
import jax.numpy as jnp
from jax import lax

D = 4096
HEAD_DIM = 64
IN_LEN = 384
OUT_LEN = 128
INNER = 3072
SOURCE_TOTAL = 3072
TARGET_TOTAL = 1024
N_SECTION = 8
N_FSDP = 4


def draw_attn_weights(key, part):
    shape_all = (N_SECTION, 4, D, INNER)
    drawn = jnp.clip(jax.random.normal(key, shape_all, jnp.float32), -6.0, 6.0) / math.sqrt(D)
    return drawn.astype(jnp.bfloat16)


def touch_ends(array, stream_key, least, high):
    longest = array.shape.index(max(array.shape))
    spots = []
    for shift in (0, 1):
        where = [jax.random.randint(jax.random.fold_in(stream_key, axis), (), 0, length) for axis, length in enumerate(array.shape)]
        where[longest] = (where[longest] + shift) % array.shape[longest]
        spots.append(tuple(where))
    return array.at[spots[0]].set(least).at[spots[1]].set(high)


def block_levels(rng, extent, shards, smallest, high):
    gain, own = 1.0, jax.random.fold_in(rng, 6)
    for position, parts in shards:
        draws = jnp.exp(jax.random.uniform(jax.random.fold_in(own, position), (parts,), jnp.float32, smallest / len(shards), high / len(shards)))
        gain = gain * jnp.repeat(draws, extent[position] // parts).reshape([-1 if axis == position else 1 for axis in range(len(extent))])
    return gain


def centred(stream_key, shape, deviation, limit, split=(), kind=jnp.bfloat16):
    result = deviation * jax.random.normal(stream_key, shape, jnp.float32)
    if split:
        result = result * block_levels(stream_key, shape, split, -0.22, 0.18)
    return jnp.clip(result, -limit, limit).astype(kind)


def setup_inputs(seed: int = 0) -> dict:
    keys = jax.random.split(jax.random.key(seed), 6)
    source_rows = centred(keys[0], (SOURCE_TOTAL, D), 1.0, 6.0, ((0, 32),))
    target_rows = centred(keys[1], (TARGET_TOTAL, D), 1.0, 6.0, ((0, 8),))
    attn_weights = draw_attn_weights(jax.random.fold_in(keys[5], 71), 0)
    gains = jnp.clip(1.0 + 0.15 * jax.random.normal(keys[3], (N_SECTION, D), jnp.float32), 0.25, 1.75)
    lengths = touch_ends(jax.random.randint(keys[4], (N_SECTION,), IN_LEN // 2, IN_LEN + 1), jax.random.fold_in(keys[4], 1), IN_LEN // 2, IN_LEN).astype(jnp.int32)
    return dict(source_rows=source_rows, target_rows=target_rows, attn_weights=attn_weights, gains=gains, lengths=lengths)


def rms_norm(block_rows, gain_row):
    widened = block_rows.astype(jnp.float32)
    inverse_rms = lax.rsqrt(lax.optimization_barrier(jnp.mean(widened * widened, axis=-1, keepdims=True)) + 1e-06)
    return (widened * inverse_rms * gain_row).astype(jnp.bfloat16)

def project(block_rows, weight):
    return jnp.dot(block_rows, weight, preferred_element_type=jnp.float32).astype(jnp.bfloat16)

def attend(queries, key_rows, values, length):
    query_count = queries.shape[0]
    key_count = key_rows.shape[0]
    head_count = queries.shape[1] // HEAD_DIM
    query_heads = queries.reshape(query_count, head_count, HEAD_DIM).astype(jnp.float32)
    key_heads = key_rows.reshape(key_count, head_count, HEAD_DIM).astype(jnp.float32)
    value_heads = values.reshape(key_count, head_count, HEAD_DIM).astype(jnp.float32)
    scores = jnp.einsum('qhc,khc->hqk', query_heads, key_heads) * 0.125
    key_valid = jnp.arange(key_count, dtype=jnp.int32) < length
    scores = jnp.where(key_valid[None, None, :], scores, -1000000000.0)
    row_max = lax.optimization_barrier(jnp.max(scores, axis=-1, keepdims=True))
    expo = jnp.exp(scores - row_max)
    soft = (expo / lax.optimization_barrier(jnp.sum(expo, axis=-1, keepdims=True))).astype(jnp.bfloat16)
    context = jnp.einsum('hqk,khc->qhc', soft.astype(jnp.float32), value_heads)
    return context.reshape(query_count, head_count * HEAD_DIM).astype(jnp.bfloat16)

def out_terms(context, out_weight):
    row_count = context.shape[0]
    context_groups = context.reshape(row_count, N_FSDP, -1).astype(jnp.float32)
    weight_groups = out_weight.reshape(out_weight.shape[0], N_FSDP, -1).astype(jnp.float32)
    group_terms = jnp.einsum('rgc,dgc->grd', context_groups, weight_groups)
    rounded = lax.optimization_barrier(group_terms.astype(jnp.bfloat16))
    return lax.optimization_barrier(jnp.sum(rounded.astype(jnp.float32), axis=0))

def reference(source_rows, target_rows, attn_weights, gains, lengths):
    half_sections = N_SECTION // 2
    source_blocks = source_rows.reshape(N_SECTION, IN_LEN, D)
    target_blocks = target_rows.reshape(N_SECTION, OUT_LEN, D)
    source_out = []
    target_out = []
    for section_index in range(N_SECTION):
        weights = attn_weights[section_index]
        gain_row = gains[section_index]
        length = lengths[section_index]
        source_block = source_blocks[section_index]
        target_block = target_blocks[section_index]
        if section_index < half_sections:
            normed = rms_norm(source_block, gain_row)
            context = attend(project(normed, weights[0]), project(normed, weights[1]), project(normed, weights[2]), length)
            source_block = (source_block.astype(jnp.float32) + out_terms(context, weights[3])).astype(jnp.bfloat16)
        else:
            normed = rms_norm(target_block, gain_row)
            context = attend(project(normed, weights[0]), project(source_block, weights[1]), project(source_block, weights[2]), length)
            target_block = (target_block.astype(jnp.float32) + out_terms(context, weights[3])).astype(jnp.bfloat16)
        source_out.append(source_block)
        target_out.append(target_block)
    source_next = jnp.roll(jnp.stack(source_out), 1, axis=0).reshape(N_SECTION * IN_LEN, D)
    target_next = jnp.roll(jnp.stack(target_out), 1, axis=0).reshape(N_SECTION * OUT_LEN, D)
    return (source_next, target_next)
```

```python
import functools
import math

import jax
import jax.numpy as jnp
from jax import lax
from jax.experimental import pallas as pl
from jax.experimental.pallas import tpu as pltpu
from jax.sharding import PartitionSpec as P

HEAD_DIM = 64
BLOCKS = 8
CUTS = 2
GATHER = (2, 2, 2, 2, 2, 2, 1, 1, 1, 1)
LEAD = (("O", 0), ("O", 1), ("O", 2), ("S", 0))
TRAIL = (
    ("S", 1), ("S", 2), ("W", 0), ("W", 1), ("O", 3), ("F", 0), ("O", 4), ("F", 1), ("S", 3),
    ("W", 2), ("F", 2), ("W", 3), ("O", 5), ("S", 4), ("F", 3), ("O", 6), ("W", 4), ("F", 4),
    ("S", 5), ("O", 7), ("F", 5), ("W", 5), ("S", 6), ("F", 6), ("W", 6), ("S", 7), ("F", 7),
    ("W", 7),
) + tuple(("F", j) for j in range(8, BLOCKS * CUTS))
F32 = jnp.float32
BF16 = jnp.bfloat16


def rms_norm(block, gain):
    wide = block.astype(F32)
    inverse = lax.rsqrt(jnp.mean(wide * wide, axis=-1, keepdims=True) + 1e-06)
    return (wide * inverse * gain).astype(BF16)


def spans_of(parts, d):
    unit = d // sum(parts)
    return [(sum(parts[:j]) * unit, part * unit) for j, part in enumerate(parts)]


def chunk_of(count):
    return 32 if count % 32 == 0 else 16


def kernel(
    n_sec, n_f, x_hbm, y_hbm, gain_hbm, len_hbm, w_hbm, so, to,
    xin, yin, gain_ref, len_ref, xs, ny, w, acc, qkv, ctx, term, prt, sums, rem, own, prt_own, fin,
    dterm, dprt, dp, yfin,
    x_sem, y_sem, g_sem, w_sem, ag_s, ag_r, pt_s, pt_r, fw_s, fw_r, t1_s, t1_r, x1_s, x1_r,
    t2_s, t2_r, ss_s, ss_r, ts_s, ts_r, tf_s, tf_r,
):
    chips = n_f // 2
    rows, d = xin.shape
    pair = 2 * rows
    total = pair * chips
    t_rows = yin.shape[0]
    t_half = t_rows // 2
    width = w.shape[2]
    spans = spans_of(GATHER, d)
    n_g, n_p = len(spans), BLOCKS
    cn, fn = d // BLOCKS, d // (BLOCKS * CUTS)
    sec, f = lax.axis_index("section"), lax.axis_index("fsdp")
    core, chip = lax.rem(f, 2), f // 2
    other = 1 - core
    enc = sec < n_sec // 2
    dec = jnp.logical_not(enc)
    partner = {"fsdp": chip * 2 + other}
    nxt = {"section": lax.rem(sec + 1, n_sec)}
    prv = {"section": lax.rem(sec + n_sec - 1, n_sec)}

    def ahead(k):
        return lax.rem(chip + k, chips)

    def behind(k):
        return lax.rem(chip + chips - k, chips)

    def peer(h):
        return {"fsdp": h * 2 + core}

    def remote(src, dst, send, recv, dev):
        return pltpu.make_async_remote_copy(
            src_ref=src, dst_ref=dst, send_sem=send, recv_sem=recv,
            device_id=dev, device_id_type=pl.DeviceIdType.MESH,
        )

    def at(start, size):
        return pl.ds(pl.multiple_of(start, 16), size)

    def cols(j):
        return pl.ds(j * cn, cn)

    def fine(j):
        return pl.ds(j * fn, fn)

    barrier = pltpu.get_barrier_semaphore()
    greet = [partner, prv] + [peer(ahead(k)) for k in range(1, chips)]
    with jax.named_scope("signal"):
        for dev in greet:
            pl.semaphore_signal(barrier, inc=1, device_id=dev, device_id_type=pl.DeviceIdType.MESH)

    x_rows, y_rows = chunk_of(rows), chunk_of(t_rows)
    gain_copy = pltpu.make_async_copy(gain_hbm, gain_ref, g_sem.at[0])
    len_copy = pltpu.make_async_copy(len_hbm, len_ref, g_sem.at[1])
    y_copy = pltpu.make_async_copy(y_hbm, yin, y_sem)
    w_copies = [pltpu.make_async_copy(w_hbm.at[0, i], w.at[i], w_sem.at[i]) for i in range(4)]
    x_copy = pltpu.make_async_copy(x_hbm, xin, x_sem)
    gain_copy.start()
    x_copy.start()
    y_copy.start()
    gain_copy.wait()
    gain = gain_ref[...]
    with jax.named_scope("x_wait"):
        x_copy.wait()
    for cp in w_copies:
        cp.start()
    len_copy.start()

    def block(h, which):
        return at((h * 2 + which) * rows, rows)

    @pl.when(enc)
    def _():
        def step(r, carry):
            xs[at(f * rows + r * x_rows, x_rows), :] = rms_norm(
                xin[at(r * x_rows, x_rows), :], gain
            )
            return carry

        lax.fori_loop(0, rows // x_rows, step, 0)

    @pl.when(dec)
    def _():
        xs[at(f * rows, rows), :] = xin[...]

    with jax.named_scope("barrier_wait"):
        pl.semaphore_wait(barrier, len(greet))

    def gather_send(k, j):
        spot = xs.at[block(chip, core), pl.ds(*spans[j])]
        return remote(spot, spot, ag_s.at[k - 1], ag_r.at[k - 1, j], peer(ahead(k)))

    def gather_recv(k, j):
        spot = xs.at[block(behind(k), core), pl.ds(*spans[j])]
        return remote(spot, spot, ag_s.at[k - 1], ag_r.at[k - 1, j], peer(behind(k)))

    def forward(k, j, which):
        spot = xs.at[block(behind(k), which), pl.ds(*spans[j])]
        return remote(spot, spot, fw_s.at[k - 1], fw_r.at[k - 1, j], partner)

    def swap(which):
        spot = xs.at[block(chip, which), :]
        return remote(spot, spot, pt_s, pt_r, partner)

    for j in range(n_g):
        for k in range(1, chips):
            gather_send(k, j).start()
    swap(core).start()

    def shift_source(j, src):
        return remote(src.at[:, fine(j)], so.at[:, fine(j)], ss_s, ss_r, nxt)

    def half(which):
        return at(which * t_half, t_half)

    def shift_target(j, src):
        return remote(src, to.at[half(core), cols(j)], ts_s, ts_r.at[j], nxt)

    with jax.named_scope("y_wait"):
        y_copy.wait()

    @pl.when(enc)
    def _():
        for j in range(n_p):
            shift_target(j, yin.at[half(core), cols(j)]).start()

    @pl.when(dec)
    def _():
        for j in range(n_p * CUTS):
            shift_source(j, xin).start()

    scales = (HEAD_DIM**-0.5 * math.log2(math.e), None, None)

    def store(which, start, count, value):
        if scales[which] is not None:
            value = value * scales[which]
        qkv[which, at(start, count), :] = value.astype(BF16)

    def project(src, which, start, count):
        store(which, start, count, jnp.dot(src, w[which], preferred_element_type=F32))

    def project_piece(which, h, j):
        lanes = pl.ds(*spans[j])
        part = jnp.dot(
            xs[at(h * pair, pair), lanes], w[which, lanes, :], preferred_element_type=F32
        )
        if j:
            part = part + acc[which]
        if j < n_g - 1:
            acc[which] = part
        else:
            store(which, h * pair, pair, part)

    @pl.when(dec)
    def _():
        def step(r, carry):
            spot = at(r * y_rows, y_rows)
            ny[spot, :] = rms_norm(yin[spot, :], gain)
            return carry

        lax.fori_loop(0, t_rows // y_rows, step, 0)

    with jax.named_scope("wait_w0"):
        w_copies[0].wait()

    @pl.when(dec)
    def _():
        with jax.named_scope("proj_ny"):
            project(ny[...], 0, 0, t_rows)

    with jax.named_scope("wait_swap"):
        swap(other).wait_recv()

    @pl.when(enc)
    def _():
        with jax.named_scope("proj_q"):
            project(xs[at(chip * pair, pair), :], 0, chip * pair, pair)

    for which in (1, 2):
        with jax.named_scope(f"wait_w{which}"):
            w_copies[which].wait()
        with jax.named_scope(f"proj_{which}"):
            project(xs[at(chip * pair, pair), :], which, chip * pair, pair)

    def consume(k, j):
        with jax.named_scope(f"fwait{j}"):
            forward(k, j, other).wait_recv()

        @pl.when(enc)
        def _():
            with jax.named_scope(f"pp0_{j}"):
                project_piece(0, behind(k), j)

        with jax.named_scope(f"pp12_{j}"):
            project_piece(1, behind(k), j)
            project_piece(2, behind(k), j)

    arrivals = [(k, j) for k in range(1, chips) for j in range(n_g)]
    for n, (k, j) in enumerate(arrivals):
        with jax.named_scope(f"gwait{j}"):
            gather_recv(k, j).wait_recv()
        forward(k, j, core).start()
        if n:
            consume(*arrivals[n - 1])
    if arrivals:
        consume(*arrivals[-1])

    with jax.named_scope("wait_len"):
        len_copy.wait()
    length = len_ref[0]

    def attend(start, count):
        sure = total // 2 // 128 * 128
        key_ok = sure + lax.broadcasted_iota(jnp.int32, (1, total - sure), 1) < length
        first = lax.broadcasted_iota(jnp.int32, (1, 2 * HEAD_DIM), 1) < HEAD_DIM
        ones = jnp.ones((total, 2 * HEAD_DIM), BF16)

        def step(t, carry):
            lanes = pl.ds(pl.multiple_of(t * 2 * HEAD_DIM, 128), 2 * HEAD_DIM)
            queries = qkv[0, at(start, count), lanes]
            keys = qkv[1, :total, lanes]
            values = jnp.concatenate([qkv[2, :total, lanes], ones], axis=1)
            zero = jnp.zeros_like(queries)
            both = jnp.concatenate(
                [jnp.where(first, queries, zero), jnp.where(first, zero, queries)], axis=0
            )
            scores = lax.dot_general(
                both, keys, (((1,), (1,)), ((), ())), preferred_element_type=F32
            )
            tail = jnp.where(key_ok, scores[:, sure:], -1000000000.0 * math.log2(math.e))
            if sure:
                scores = jnp.concatenate([scores[:, :sure], tail], axis=1)
            else:
                scores = tail
            expo = jnp.exp2(scores - jnp.max(scores, axis=-1, keepdims=True)).astype(BF16)
            mixed = jnp.dot(expo, values, preferred_element_type=F32)
            mixed = mixed[:, : 2 * HEAD_DIM] * (1.0 / mixed[:, 2 * HEAD_DIM :])
            ctx[at(start, count), lanes] = jnp.where(
                first, mixed[:count], mixed[count:]
            ).astype(BF16)
            return carry

        with jax.named_scope("attend"):
            lax.fori_loop(0, width // (2 * HEAD_DIM), step, 0, unroll=True)

    def out_piece(start, count, dst, j):
        with jax.named_scope("outp"):
            dst[:, cols(j)] = lax.dot_general(
                ctx[at(start, count), :], w[3, cols(j), :], (((1,), (1,)), ((), ())),
                preferred_element_type=F32,
            ).astype(BF16)

    def mate_term(k, j):
        return remote(
            term.at[k - 1, at(other * rows, rows), cols(j)], prt.at[k - 1, :, cols(j)],
            t1_s.at[k - 1], t1_r.at[k - 1, j], partner,
        )

    def send_sum(k, j):
        return remote(
            sums.at[k - 1, :, fine(j)], rem.at[k - 1, :, fine(j)],
            x1_s.at[k - 1], x1_r.at[k - 1, j], peer(ahead(k)),
        )

    def mate_own(j):
        return remote(
            own.at[at(other * rows, rows), cols(j)], prt_own.at[:, cols(j)],
            t2_s, t2_r.at[j], partner,
        )

    def mate_target(j):
        return remote(
            dterm.at[half(other), cols(j)], dprt.at[:, cols(j)], t1_s.at[0], t1_r.at[0, j], partner
        )

    def send_target(k, j):
        return remote(
            dp.at[chip, :, cols(j)], dp.at[chip, :, cols(j)],
            x1_s.at[k - 1], x1_r.at[k - 1, j], peer(ahead(k)),
        )

    def recv_target(k, j):
        spot = dp.at[behind(k), :, cols(j)]
        return remote(spot, spot, x1_s.at[k - 1], x1_r.at[k - 1, j], peer(behind(k)))

    with jax.named_scope("wait_w3"):
        w_copies[3].wait()

    @pl.when(enc)
    def _():
        def term_piece(k, j):
            out_piece(ahead(k) * pair, pair, term.at[k - 1], j)
            mate_term(k, j).start()

        def pass_on(k, j):
            with jax.named_scope("mtw"):
                mate_term(k, j).wait_recv()
            mine = term[k - 1, at(core * rows, rows), cols(j)].astype(F32)
            sums[k - 1, :, cols(j)] = (mine + prt[k - 1, :, cols(j)].astype(F32)).astype(BF16)
            for cut in range(CUTS):
                send_sum(k, j * CUTS + cut).start()

        def own_piece(j):
            out_piece(chip * pair, pair, own, j)
            mate_own(j).start()

        def finish(j):
            if j % CUTS == 0:
                with jax.named_scope("mow"):
                    mate_own(j // CUTS).wait_recv()
            delta = own[at(core * rows, rows), fine(j)].astype(F32) + prt_own[:, fine(j)].astype(F32)
            for k in range(1, chips):
                with jax.named_scope(f"ssw{j}"):
                    send_sum(k, j).wait_recv()
                delta += rem[k - 1, :, fine(j)].astype(F32)
            fin[:, fine(j)] = (xin[:, fine(j)].astype(F32) + delta).astype(BF16)
            shift_source(j, fin).start()

        for k in range(1, chips - 1):
            attend(ahead(k) * pair, pair)
            for j in range(n_p):
                term_piece(k, j)
                if j:
                    pass_on(k, j - 1)
            pass_on(k, n_p - 1)

        last = chips - 1
        acts = {"O": lambda j: term_piece(last, j), "S": lambda j: pass_on(last, j),
                "W": own_piece, "F": finish}
        if last:
            attend(ahead(last) * pair, pair)
            for name, j in LEAD:
                acts[name](j)
        attend(chip * pair, pair)
        for name, j in TRAIL:
            if last or name in "WF":
                acts[name](j)
        whole = pl.ds(0, rows)
        remote(own.at[whole], prt_own, t2_s, t2_r.at[0], partner).wait_send()
        for k in range(1, chips):
            remote(
                term.at[k - 1, whole], prt.at[k - 1], t1_s.at[k - 1], t1_r.at[k - 1, 0], partner
            ).wait_send()
            remote(
                sums.at[k - 1], rem.at[k - 1], x1_s.at[k - 1], x1_r.at[k - 1, 0], peer(ahead(k))
            ).wait_send()

    @pl.when(dec)
    def _():
        attend(0, t_rows)

        def pass_on(j):
            with jax.named_scope("mtgw"):
                mate_target(j).wait_recv()
            mine = dterm[half(core), cols(j)].astype(F32)
            dp[chip, :, cols(j)] = (mine + dprt[:, cols(j)].astype(F32)).astype(BF16)
            for k in range(1, chips):
                send_target(k, j).start()

        for j in range(n_p):
            out_piece(0, t_rows, dterm, j)
            mate_target(j).start()
            if j > 2:
                pass_on(j - 3)
        for j in range(n_p - 3, n_p):
            pass_on(j)
        for j in range(n_p):
            for k in range(1, chips):
                with jax.named_scope(f"rtw{j}"):
                    recv_target(k, j).wait_recv()
            delta = dp[0, :, cols(j)].astype(F32)
            for h in range(1, chips):
                delta += dp[h, :, cols(j)].astype(F32)
            yfin[:, cols(j)] = (yin[half(core), cols(j)].astype(F32) + delta).astype(BF16)
            shift_target(j, yfin.at[:, cols(j)]).start()
        remote(dterm.at[half(other)], dprt, t1_s.at[0], t1_r.at[0, 0], partner).wait_send()
        for k in range(1, chips):
            remote(
                dp.at[chip], dp.at[chip], x1_s.at[k - 1], x1_r.at[k - 1, 0], peer(ahead(k))
            ).wait_send()

    def cross(which, lanes):
        spot = to.at[half(which), lanes]
        return remote(spot, spot, tf_s, tf_r, partner)

    for j in range(n_p):
        with jax.named_scope(f"stw{j}"):
            shift_target(j, yfin.at[:, cols(j)]).wait_recv()
        cross(core, cols(j)).start()
    every = pl.ds(0, d)
    shifted = remote(fin, so, ss_s, ss_r, nxt)
    with jax.named_scope("shw"):
        shifted.wait_recv()
    with jax.named_scope("crw"):
        cross(other, every).wait_recv()

    with jax.named_scope("end"):
        swap(core).wait_send()
        for k in range(1, chips):
            mine, theirs = xs.at[block(chip, core)], xs.at[block(behind(k), core)]
            remote(mine, mine, ag_s.at[k - 1], ag_r.at[k - 1, 0], peer(ahead(k))).wait_send()
            remote(theirs, theirs, fw_s.at[k - 1], fw_r.at[k - 1, 0], partner).wait_send()
        shifted.wait_send()
        remote(yfin, to.at[half(core)], ts_s, ts_r.at[0], nxt).wait_send()
        cross(core, every).wait_send()


def local(n_sec, n_f, source_rows, target_rows, attn_weights, gains, lengths):
    chips = n_f // 2
    more = max(chips - 1, 1)
    rows, d = source_rows.shape
    t_rows = target_rows.shape[0]
    width = attn_weights.shape[3]
    pair, total, t_half = 2 * rows, rows * n_f, t_rows // 2
    q_rows = max(total, t_rows)
    n_g, n_p = len(GATHER), BLOCKS
    dma = pltpu.SemaphoreType.DMA
    vmem = lambda *shape: pltpu.VMEM(shape, BF16)
    scratch = [
        vmem(rows, d), vmem(t_rows, d), pltpu.VMEM((1, d), F32), pltpu.SMEM((1,), jnp.int32),
        vmem(total, d), vmem(t_rows, d), vmem(4, d, width), pltpu.VMEM((3, pair, width), F32),
        vmem(3, q_rows, width), vmem(q_rows, width),
        vmem(more, pair, d), vmem(more, rows, d), vmem(more, rows, d), vmem(more, rows, d),
        vmem(pair, d), vmem(rows, d), vmem(rows, d),
        vmem(t_rows, d), vmem(t_half, d), vmem(chips, t_half, d), vmem(t_half, d),
        dma, dma, dma((2,)),
        dma((4,)), dma((more,)), dma((more, n_g)), dma, dma, dma((more,)), dma((more, n_g)),
        dma((more,)), dma((more, n_p)), dma((more,)), dma((more, n_p * CUTS)), dma, dma((n_p,)),
        dma, dma, dma, dma((n_p,)), dma, dma,
    ]
    anywhere = pl.BlockSpec(memory_space=pl.ANY)
    moved = pl.pallas_call(
        functools.partial(kernel, n_sec, n_f),
        out_shape=(
            pltpu.VMEM(source_rows.shape, BF16),
            pltpu.VMEM(target_rows.shape, BF16),
        ),
        in_specs=[anywhere] * 5,
        out_specs=(anywhere, anywhere),
        scratch_shapes=scratch,
        compiler_params=pltpu.CompilerParams(
            collective_id=0, has_side_effects=True, vmem_limit_bytes=56 * 1024 * 1024
        ),
    )(source_rows, target_rows, gains, lengths, attn_weights)
    return settle(*moved)


def settle(source, target):
    def body(a_ref, b_ref, a_out, b_out, sem):
        plan = []
        for src, dst in ((a_ref, a_out), (b_ref, b_out)):
            step = src.shape[1] // 4
            for j in range(4):
                lanes = pl.ds(j * step, step)
                plan.append(pltpu.make_async_copy(src.at[:, lanes], dst.at[:, lanes], sem.at[len(plan)]))
        for copy in plan:
            copy.start()
        for copy in plan:
            copy.wait()

    anywhere = pl.BlockSpec(memory_space=pl.ANY)
    return pl.pallas_call(
        body,
        out_shape=tuple(jax.ShapeDtypeStruct(v.shape, v.dtype) for v in (source, target)),
        in_specs=[anywhere, anywhere],
        out_specs=(anywhere, anywhere),
        scratch_shapes=[pltpu.SemaphoreType.DMA((8,))],
        compiler_params=pltpu.CompilerParams(vmem_limit_bytes=8 * 1024 * 1024),
    )(source, target)


def solution(mesh):
    in_specs = (
        P(("section", "fsdp"), None),
        P("section", None),
        P("section", None, None, "fsdp"),
        P("section", None),
        P("section"),
    )
    out_specs = (P(("section", "fsdp"), None), P("section", None))
    body = functools.partial(local, mesh.shape["section"], mesh.shape["fsdp"])
    return jax.shard_map(body, mesh=mesh, in_specs=in_specs, out_specs=out_specs, check_vma=False)
```

```python
import functools
import math

import jax
import jax.numpy as jnp
from jax import lax
from jax.experimental import pallas as pl
from jax.experimental.pallas import tpu as pltpu
from jax.sharding import PartitionSpec as P

HEAD_DIM = 64
BLOCKS = 8
CUTS = (4,) + (2,) * (BLOCKS - 1)
GATHER = (4, 2, 2, 2, 2, 1, 1, 1, 1)
MOVED = 2
LEAD = (("O", 1), ("S", 0))
TRAIL = (
    ("S", 1), ("O", 2), ("F", 0), ("W", 1), ("F", 1), ("O", 3), ("F", 2), ("F", 3), ("S", 2),
    ("O", 4), ("W", 2), ("S", 3), ("F", 4), ("O", 5), ("F", 5), ("W", 3), ("S", 4), ("F", 6),
    ("O", 6), ("F", 7), ("S", 5), ("W", 4), ("F", 8), ("O", 7), ("F", 9), ("S", 6), ("W", 5),
    ("F", 10), ("W", 6), ("F", 11), ("S", 7), ("F", 12), ("W", 7),
) + tuple(("F", j) for j in range(13, sum(CUTS)))
F32 = jnp.float32
BF16 = jnp.bfloat16


def rms_norm(block, gain):
    wide = block.astype(F32)
    inverse = lax.rsqrt(jnp.mean(wide * wide, axis=-1, keepdims=True) + 1e-06)
    return (wide * inverse * gain).astype(BF16)


def spans_of(parts, d):
    unit = d // sum(parts)
    return [(sum(parts[:j]) * unit, part * unit) for j, part in enumerate(parts)]


def chunk_of(count):
    return 32 if count % 32 == 0 else 16


def kernel(
    n_sec, n_f, x_hbm, y_hbm, gain_hbm, len_hbm, w_hbm, so, to,
    xin, yin, gain_ref, len_ref, xs, ny, w, acc, qkv, ctx, term, prt, sums, rem, own, prt_own, fin,
    dterm, dprt, dp, yfin,
    x_sem, y_sem, g_sem, w_sem, ag_s, ag_r, pt_s, pt_r, fw_s, fw_r, mv_s, t1_s, t1_r, x1_s, x1_r,
    t2_s, t2_r, ss_s, ss_r, ts_s, ts_r, tf_s, tf_r,
):
    chips = n_f // 2
    rows, d = xin.shape
    pair = 2 * rows
    total = pair * chips
    t_rows = yin.shape[0]
    t_half = t_rows // 2
    width = w.shape[2]
    spans = spans_of(GATHER, d)
    n_g, n_p = len(spans), BLOCKS
    cn = d // BLOCKS
    cuts = [(b, c) for b in range(BLOCKS) for c in range(CUTS[b])]
    sec, f = lax.axis_index("section"), lax.axis_index("fsdp")
    core, chip = lax.rem(f, 2), f // 2
    other = 1 - core
    enc = sec < n_sec // 2
    even, odd = core == 0, core == 1
    dec = jnp.logical_not(enc)
    partner = {"fsdp": chip * 2 + other}
    nxt = {"section": lax.rem(sec + 1, n_sec)}
    prv = {"section": lax.rem(sec + n_sec - 1, n_sec)}

    def ahead(k):
        return lax.rem(chip + k, chips)

    def behind(k):
        return lax.rem(chip + chips - k, chips)

    def peer(h):
        return {"fsdp": h * 2 + core}

    def remote(src, dst, send, recv, dev):
        return pltpu.make_async_remote_copy(
            src_ref=src, dst_ref=dst, send_sem=send, recv_sem=recv,
            device_id=dev, device_id_type=pl.DeviceIdType.MESH,
        )

    def at(start, size):
        return pl.ds(pl.multiple_of(start, 16), size)

    def cols(j):
        return pl.ds(j * cn, cn)

    def fine(j):
        b, c = cuts[j]
        return pl.ds(b * cn + c * (cn // CUTS[b]), cn // CUTS[b])

    barrier = pltpu.get_barrier_semaphore()
    greet = [partner, prv] + [peer(ahead(k)) for k in range(1, chips)]
    with jax.named_scope("signal"):
        for dev in greet:
            pl.semaphore_signal(barrier, inc=1, device_id=dev, device_id_type=pl.DeviceIdType.MESH)

    x_rows, y_rows = chunk_of(rows), chunk_of(t_rows)
    gain_copy = pltpu.make_async_copy(gain_hbm, gain_ref, g_sem.at[0])
    len_copy = pltpu.make_async_copy(len_hbm, len_ref, g_sem.at[1])
    y_copy = pltpu.make_async_copy(y_hbm, yin, y_sem)
    w_copies = [pltpu.make_async_copy(w_hbm.at[0, i], w.at[i], w_sem.at[i]) for i in range(4)]
    x_copies = [
        pltpu.make_async_copy(
            x_hbm.at[pl.ds(r * x_rows, x_rows)], xin.at[pl.ds(r * x_rows, x_rows)], x_sem.at[r]
        )
        for r in range(rows // x_rows)
    ]
    gain_copy.start()
    for cp in x_copies:
        cp.start()
    y_copy.start()
    gain_copy.wait()
    gain = gain_ref[...]

    def arrived(r):
        x_copies[r].wait()
        if r == len(x_copies) - 1:
            for cp in w_copies:
                cp.start()
            len_copy.start()

    def block(h, which):
        return at((h * 2 + which) * rows, rows)

    @pl.when(enc)
    def _():
        for r in range(len(x_copies)):
            arrived(r)
            xs[at(f * rows + r * x_rows, x_rows), :] = rms_norm(
                xin[pl.ds(r * x_rows, x_rows), :], gain
            )

    @pl.when(dec)
    def _():
        for r in range(len(x_copies)):
            arrived(r)
        xs[at(f * rows, rows), :] = xin[...]

    with jax.named_scope("barrier_wait"):
        pl.semaphore_wait(barrier, len(greet))

    def gather_send(k, j):
        spot = xs.at[block(chip, core), pl.ds(*spans[j])]
        return remote(spot, spot, ag_s.at[k - 1], ag_r.at[k - 1, j], peer(ahead(k)))

    def gather_recv(k, j):
        spot = xs.at[block(behind(k), core), pl.ds(*spans[j])]
        return remote(spot, spot, ag_s.at[k - 1], ag_r.at[k - 1, j], peer(behind(k)))

    def forward(k, j, which):
        spot = xs.at[block(behind(k), which), pl.ds(*spans[j])]
        return remote(spot, spot, fw_s.at[k - 1], fw_r.at[k - 1, j], partner)

    def moved_send(k, j):
        spot = xs.at[at(chip * pair, pair), pl.ds(*spans[j])]
        return remote(spot, spot, mv_s.at[0], ag_r.at[k - 1, j], peer(ahead(k)))

    def moved_recv(k, j):
        spot = xs.at[at(behind(k) * pair, pair), pl.ds(*spans[j])]
        return remote(spot, spot, mv_s.at[0], ag_r.at[k - 1, j], peer(behind(k)))

    def moved_forward(k, j):
        spot = xs.at[at(behind(k) * pair, pair), pl.ds(*spans[j])]
        return remote(spot, spot, mv_s.at[1], fw_r.at[k - 1, j], partner)

    def swap(which):
        spot = xs.at[block(chip, which), :]
        return remote(spot, spot, pt_s, pt_r, partner)

    kept = n_g - MOVED
    for j in range(kept):
        for k in range(1, chips):
            gather_send(k, j).start()
    swap(core).start()

    def shift_source(j, src):
        return remote(src.at[:, fine(j)], so.at[:, fine(j)], ss_s, ss_r, nxt)

    def half(which):
        return at(which * t_half, t_half)

    def shift_target(j, src):
        return remote(src, to.at[half(core), cols(j)], ts_s, ts_r.at[j // (n_p // 2)], nxt)

    with jax.named_scope("y_wait"):
        y_copy.wait()

    @pl.when(enc)
    def _():
        for j in range(n_p):
            shift_target(j, yin.at[half(core), cols(j)]).start()

    @pl.when(dec)
    def _():
        for j in range(len(cuts)):
            shift_source(j, xin).start()

    scales = (HEAD_DIM**-0.5 * math.log2(math.e), None, None)

    def store(which, start, count, value):
        if scales[which] is not None:
            value = value * scales[which]
        qkv[which, at(start, count), :] = value.astype(BF16)

    def project(src, which, start, count):
        store(which, start, count, jnp.dot(src, w[which], preferred_element_type=F32))

    def project_piece(which, h, group):
        lanes = pl.ds(spans[group[0]][0], sum(spans[j][1] for j in group))
        part = jnp.dot(
            xs[at(h * pair, pair), lanes], w[which, lanes, :], preferred_element_type=F32
        )
        if group[0]:
            part = part + acc[which]
        if group[-1] < n_g - 1:
            acc[which] = part
        else:
            store(which, h * pair, pair, part)

    @pl.when(dec)
    def _():
        def step(r, carry):
            spot = at(r * y_rows, y_rows)
            ny[spot, :] = rms_norm(yin[spot, :], gain)
            return carry

        lax.fori_loop(0, t_rows // y_rows, step, 0)

    with jax.named_scope("wait_w0"):
        w_copies[0].wait()

    @pl.when(dec)
    def _():
        with jax.named_scope("proj_ny"):
            project(ny[...], 0, 0, t_rows)

    with jax.named_scope("wait_swap"):
        swap(other).wait_recv()

    @pl.when(odd)
    def _():
        for j in range(kept, n_g):
            for k in range(1, chips):
                moved_send(k, j).start()

    @pl.when(enc)
    def _():
        with jax.named_scope("proj_q"):
            project(xs[at(chip * pair, pair), :], 0, chip * pair, pair)

    for which in (1, 2):
        with jax.named_scope(f"wait_w{which}"):
            w_copies[which].wait()
        with jax.named_scope(f"proj_{which}"):
            project(xs[at(chip * pair, pair), :], which, chip * pair, pair)

    def consume(k, *group):
        for j in group:
            with jax.named_scope(f"fwait{j}"):
                if j < kept:
                    forward(k, j, other).wait_recv()
                else:
                    @pl.when(even)
                    def _():
                        moved_forward(k, j).wait_recv()

        @pl.when(enc)
        def _():
            with jax.named_scope(f"pp0_{j}"):
                project_piece(0, behind(k), group)

        with jax.named_scope(f"pp12_{j}"):
            project_piece(1, behind(k), group)
            project_piece(2, behind(k), group)

    def receive(k, j):
        with jax.named_scope(f"gwait{j}"):
            if j < kept:
                gather_recv(k, j).wait_recv()
                forward(k, j, core).start()
            else:
                @pl.when(odd)
                def _():
                    moved_recv(k, j).wait_recv()
                    moved_forward(k, j).start()

    for k in range(1, chips):
        for j in range(kept - 1):
            receive(k, j)
            if j:
                consume(k, j - 1)
        receive(k, kept - 1)
        receive(k, kept)
        consume(k, kept - 2)
        for j in range(kept + 1, n_g):
            receive(k, j)
        consume(k, kept - 1, kept)
        for j in range(kept + 1, n_g):
            consume(k, j)

    with jax.named_scope("wait_len"):
        len_copy.wait()
    length = len_ref[0]

    def attend(start, count):
        sure = total // 2 // 128 * 128
        key_ok = sure + lax.broadcasted_iota(jnp.int32, (1, total - sure), 1) < length
        first = lax.broadcasted_iota(jnp.int32, (1, 2 * HEAD_DIM), 1) < HEAD_DIM
        ones = jnp.ones((total, 2 * HEAD_DIM), BF16)

        def score(t):
            lanes = pl.ds(t * 2 * HEAD_DIM, 2 * HEAD_DIM)
            queries = qkv[0, at(start, count), lanes]
            zero = jnp.zeros_like(queries)
            both = jnp.concatenate(
                [jnp.where(first, queries, zero), jnp.where(first, zero, queries)], axis=0
            )
            return lax.dot_general(
                both, qkv[1, :total, lanes], (((1,), (1,)), ((), ())), preferred_element_type=F32
            )

        def weigh(scores):
            tail = jnp.where(key_ok, scores[:, sure:], -1000000000.0 * math.log2(math.e))
            if sure:
                scores = jnp.concatenate([scores[:, :sure], tail], axis=1)
            else:
                scores = tail
            return jnp.exp2(scores - jnp.max(scores, axis=-1, keepdims=True)).astype(BF16)

        def mix(t, expo):
            lanes = pl.ds(t * 2 * HEAD_DIM, 2 * HEAD_DIM)
            values = jnp.concatenate([qkv[2, :total, lanes], ones], axis=1)
            mixed = jnp.dot(expo, values, preferred_element_type=F32)
            mixed = mixed[:, : 2 * HEAD_DIM] * (1.0 / mixed[:, 2 * HEAD_DIM :])
            ctx[at(start, count), lanes] = jnp.where(
                first, mixed[:count], mixed[count:]
            ).astype(BF16)

        with jax.named_scope("attend"):
            pairs = range(width // (2 * HEAD_DIM))
            scores = [score(t) for t in pairs]
            weights = [weigh(block) for block in scores]
            for t in pairs:
                mix(t, weights[t])

    def out_piece(start, count, dst, j):
        with jax.named_scope("outp"):
            dst[:, cols(j)] = lax.dot_general(
                ctx[at(start, count), :], w[3, cols(j), :], (((1,), (1,)), ((), ())),
                preferred_element_type=F32,
            ).astype(BF16)

    def mate_term(k, j):
        return remote(
            term.at[k - 1, at(other * rows, rows), cols(j)], prt.at[k - 1, :, cols(j)],
            t1_s.at[k - 1], t1_r.at[k - 1, j], partner,
        )

    def send_sum(k, j):
        return remote(
            sums.at[k - 1, :, fine(j)], rem.at[k - 1, :, fine(j)],
            x1_s.at[k - 1], x1_r.at[k - 1, j], peer(ahead(k)),
        )

    def mate_own(j):
        return remote(
            own.at[at(other * rows, rows), cols(j)], prt_own.at[:, cols(j)],
            t2_s, t2_r.at[j], partner,
        )

    def mate_target(j):
        return remote(
            dterm.at[half(other), cols(j)], dprt.at[:, cols(j)], t1_s.at[0], t1_r.at[0, j], partner
        )

    def send_target(k, j):
        return remote(
            dp.at[chip, :, cols(j)], dp.at[chip, :, cols(j)],
            x1_s.at[k - 1], x1_r.at[k - 1, j], peer(ahead(k)),
        )

    def recv_target(k, j):
        spot = dp.at[behind(k), :, cols(j)]
        return remote(spot, spot, x1_s.at[k - 1], x1_r.at[k - 1, j], peer(behind(k)))

    with jax.named_scope("wait_w3"):
        w_copies[3].wait()

    @pl.when(enc)
    def _():
        def term_piece(k, j):
            out_piece(ahead(k) * pair, pair, term.at[k - 1], j)
            mate_term(k, j).start()

        def pass_on(k, j):
            with jax.named_scope("mtw"):
                mate_term(k, j).wait_recv()
            mine = term[k - 1, at(core * rows, rows), cols(j)].astype(F32)
            sums[k - 1, :, cols(j)] = (mine + prt[k - 1, :, cols(j)].astype(F32)).astype(BF16)
            for piece, (b, _) in enumerate(cuts):
                if b == j:
                    send_sum(k, piece).start()

        def own_piece(j):
            out_piece(chip * pair, pair, own, j)
            mate_own(j).start()

        def finish(j):
            if cuts[j][1] == 0:
                with jax.named_scope("mow"):
                    mate_own(cuts[j][0]).wait_recv()
            delta = own[at(core * rows, rows), fine(j)].astype(F32) + prt_own[:, fine(j)].astype(F32)
            for k in range(1, chips):
                with jax.named_scope(f"ssw{j}"):
                    send_sum(k, j).wait_recv()
                delta += rem[k - 1, :, fine(j)].astype(F32)
            fin[:, fine(j)] = (xin[:, fine(j)].astype(F32) + delta).astype(BF16)
            shift_source(j, fin).start()

        for k in range(1, chips - 1):
            attend(ahead(k) * pair, pair)
            for j in range(n_p):
                term_piece(k, j)
                if j:
                    pass_on(k, j - 1)
            pass_on(k, n_p - 1)

        last = chips - 1
        acts = {"O": lambda j: term_piece(last, j), "S": lambda j: pass_on(last, j),
                "W": own_piece, "F": finish}
        if last:
            for which in (other, core):
                start = ahead(last) * pair + which * rows
                attend(start, rows)
                out_piece(start, rows, term.at[last - 1, at(which * rows, rows)], 0)
                if which is other:
                    mate_term(last, 0).start()
            for name, j in LEAD:
                acts[name](j)
        for which in (other, core):
            start = chip * pair + which * rows
            attend(start, rows)
            out_piece(start, rows, own.at[at(which * rows, rows)], 0)
            if which is other:
                mate_own(0).start()
        for name, j in TRAIL:
            if last or name in "WF":
                acts[name](j)
        whole = pl.ds(0, rows)
        remote(own.at[whole], prt_own, t2_s, t2_r.at[0], partner).wait_send()
        for k in range(1, chips):
            remote(
                term.at[k - 1, whole], prt.at[k - 1], t1_s.at[k - 1], t1_r.at[k - 1, 0], partner
            ).wait_send()
            remote(
                sums.at[k - 1], rem.at[k - 1], x1_s.at[k - 1], x1_r.at[k - 1, 0], peer(ahead(k))
            ).wait_send()

    @pl.when(dec)
    def _():
        attend(0, t_rows)

        def pass_on(j):
            with jax.named_scope("mtgw"):
                mate_target(j).wait_recv()
            mine = dterm[half(core), cols(j)].astype(F32)
            dp[chip, :, cols(j)] = (mine + dprt[:, cols(j)].astype(F32)).astype(BF16)
            for k in range(1, chips):
                send_target(k, j).start()

        for j in range(n_p):
            out_piece(0, t_rows, dterm, j)
            mate_target(j).start()
            if j > 2:
                pass_on(j - 3)
        for j in range(n_p - 3, n_p):
            pass_on(j)
        for j in range(n_p):
            for k in range(1, chips):
                with jax.named_scope(f"rtw{j}"):
                    recv_target(k, j).wait_recv()
            delta = dp[0, :, cols(j)].astype(F32)
            for h in range(1, chips):
                delta += dp[h, :, cols(j)].astype(F32)
            yfin[:, cols(j)] = (yin[half(core), cols(j)].astype(F32) + delta).astype(BF16)
            shift_target(j, yfin.at[:, cols(j)]).start()
        remote(dterm.at[half(other)], dprt, t1_s.at[0], t1_r.at[0, 0], partner).wait_send()
        for k in range(1, chips):
            remote(
                dp.at[chip], dp.at[chip], x1_s.at[k - 1], x1_r.at[k - 1, 0], peer(ahead(k))
            ).wait_send()

    def cross(which, lanes):
        spot = to.at[half(which), lanes]
        return remote(spot, spot, tf_s, tf_r, partner)

    for j in range(2):
        part = pl.ds(j * (d // 2), d // 2)
        with jax.named_scope(f"stw{j}"):
            remote(yfin.at[:, part], to.at[half(core), part], ts_s, ts_r.at[j], nxt).wait_recv()
        cross(core, part).start()
    every = pl.ds(0, d)
    shifted = remote(fin, so, ss_s, ss_r, nxt)
    with jax.named_scope("shw"):
        shifted.wait_recv()
    with jax.named_scope("crw"):
        cross(other, every).wait_recv()

    with jax.named_scope("end"):
        swap(core).wait_send()
        for k in range(1, chips):
            sent = pl.ds(0, spans[kept][0])
            mine, theirs = xs.at[block(chip, core), sent], xs.at[block(behind(k), core), sent]
            remote(mine, mine, ag_s.at[k - 1], ag_r.at[k - 1, 0], peer(ahead(k))).wait_send()
            remote(theirs, theirs, fw_s.at[k - 1], fw_r.at[k - 1, 0], partner).wait_send()
        if chips > 1:
            late = pl.ds(0, d - spans[kept][0])

            @pl.when(odd)
            def _():
                for way, dev in ((0, peer(ahead(1))), (1, partner)):
                    spot = xs.at[pl.ds(0, total - pair), late]
                    remote(spot, spot, mv_s.at[way], fw_r.at[0, 0], dev).wait_send()

        shifted.wait_send()
        remote(yfin, to.at[half(core)], ts_s, ts_r.at[0], nxt).wait_send()
        cross(core, every).wait_send()


def local(n_sec, n_f, source_rows, target_rows, attn_weights, gains, lengths):
    chips = n_f // 2
    more = max(chips - 1, 1)
    rows, d = source_rows.shape
    t_rows = target_rows.shape[0]
    width = attn_weights.shape[3]
    pair, total, t_half = 2 * rows, rows * n_f, t_rows // 2
    q_rows = max(total, t_rows)
    n_g, n_p = len(GATHER), BLOCKS
    dma = pltpu.SemaphoreType.DMA
    vmem = lambda *shape: pltpu.VMEM(shape, BF16)
    scratch = [
        vmem(rows, d), vmem(t_rows, d), pltpu.VMEM((1, d), F32), pltpu.SMEM((1,), jnp.int32),
        vmem(total, d), vmem(t_rows, d), vmem(4, d, width), pltpu.VMEM((3, pair, width), F32),
        vmem(3, q_rows, width), vmem(q_rows, width),
        vmem(more, pair, d), vmem(more, rows, d), vmem(more, rows, d), vmem(more, rows, d),
        vmem(pair, d), vmem(rows, d), vmem(rows, d),
        vmem(t_rows, d), vmem(t_half, d), vmem(chips, t_half, d), vmem(t_half, d),
        dma((rows // chunk_of(rows),)), dma, dma((2,)),
        dma((4,)), dma((more,)), dma((more, n_g)), dma, dma, dma((more,)), dma((more, n_g)), dma((2,)),
        dma((more,)), dma((more, n_p)), dma((more,)), dma((more, sum(CUTS))), dma, dma((n_p,)),
        dma, dma, dma, dma((2,)), dma, dma,
    ]
    anywhere = pl.BlockSpec(memory_space=pl.ANY)
    moved = pl.pallas_call(
        functools.partial(kernel, n_sec, n_f),
        out_shape=(
            pltpu.VMEM(source_rows.shape, BF16),
            pltpu.VMEM(target_rows.shape, BF16),
        ),
        in_specs=[anywhere] * 5,
        out_specs=(anywhere, anywhere),
        scratch_shapes=scratch,
        compiler_params=pltpu.CompilerParams(
            collective_id=0, has_side_effects=True, vmem_limit_bytes=56 * 1024 * 1024
        ),
    )(source_rows, target_rows, gains, lengths, attn_weights)
    return settle(*moved)


def settle(source, target):
    def body(a_ref, b_ref, a_out, b_out, sem):
        plan = []
        for src, dst in ((a_ref, a_out), (b_ref, b_out)):
            step = src.shape[0] // 2
            for j in range(2):
                some = pl.ds(j * step, step)
                plan.append(pltpu.make_async_copy(src.at[some], dst.at[some], sem.at[len(plan)]))
        for copy in plan:
            copy.start()
        for copy in plan:
            copy.wait()

    anywhere = pl.BlockSpec(memory_space=pl.ANY)
    return pl.pallas_call(
        body,
        out_shape=tuple(jax.ShapeDtypeStruct(v.shape, v.dtype) for v in (source, target)),
        in_specs=[anywhere, anywhere],
        out_specs=(anywhere, anywhere),
        scratch_shapes=[pltpu.SemaphoreType.DMA((4,))],
        compiler_params=pltpu.CompilerParams(vmem_limit_bytes=8 * 1024 * 1024),
    )(source, target)


def solution(mesh):
    in_specs = (
        P(("section", "fsdp"), None),
        P("section", None),
        P("section", None, None, "fsdp"),
        P("section", None),
        P("section"),
    )
    out_specs = (P(("section", "fsdp"), None), P("section", None))
    body = functools.partial(local, mesh.shape["section"], mesh.shape["fsdp"])
    return jax.shard_map(body, mesh=mesh, in_specs=in_specs, out_specs=out_specs, check_vma=False)
```

```python
import functools
import math

import jax
import jax.numpy as jnp
from jax import lax
from jax.experimental import pallas as pl
from jax.experimental.pallas import tpu as pltpu
from jax.sharding import PartitionSpec as P

HEAD_DIM = 64
BLOCKS = 8
CUTS = (4,) + (2,) * (BLOCKS - 1)
GATHER = (4, 4, 2, 2, 1, 1, 1, 1)
MOVED = 2
LEAD = (("O", 1), ("S", 0), ("O", 2))
TRAIL = (
    ("S", 2), ("W", 1), ("F", 0), ("F", 1), ("O", 3), ("F", 2), ("F", 3), ("W", 2), ("O", 4),
    ("S", 3), ("F", 4), ("O", 5), ("F", 5), ("S", 4), ("W", 3), ("F", 6), ("O", 6), ("F", 7),
    ("S", 5), ("W", 4), ("F", 8), ("O", 7), ("F", 9), ("S", 6), ("W", 5), ("F", 10), ("S", 7),
    ("W", 6), ("F", 11), ("F", 12), ("W", 7),
) + tuple(("F", j) for j in range(13, sum(CUTS)))
F32 = jnp.float32
BF16 = jnp.bfloat16


def rms_norm(block, gain):
    wide = block.astype(F32)
    inverse = lax.rsqrt(jnp.mean(wide * wide, axis=-1, keepdims=True) + 1e-06)
    return (wide * inverse * gain).astype(BF16)


def spans_of(parts, d):
    unit = d // sum(parts)
    return [(sum(parts[:j]) * unit, part * unit) for j, part in enumerate(parts)]


def chunk_of(count):
    return 32 if count % 32 == 0 else 16


def kernel(
    n_sec, n_f, x_hbm, y_hbm, gain_hbm, len_hbm, w_hbm, so, to,
    xin, yin, gain_ref, len_ref, xs, ny, w, wt, acc, qkv, ctx, term, prt, sums, rem, own, prt_own, fin,
    dterm, dprt, dp, yfin,
    load, ag_s, ag_r, pt_s, pt_r, fw_s, fw_r, mv_s, t1_s, x1_s, x1_r,
    t2_s, ss_s, ss_r, ts_s, ts_r, tf_s, tf_r,
):
    chips = n_f // 2
    rows, d = xin.shape
    pair = 2 * rows
    total = pair * chips
    t_rows = yin.shape[0]
    t_half = t_rows // 2
    width = w.shape[2]
    spans = spans_of(GATHER, d)
    n_g, n_p = len(spans), BLOCKS
    cn = d // BLOCKS
    cuts = [(b, c) for b in range(BLOCKS) for c in range(CUTS[b])]
    sec, f = lax.axis_index("section"), lax.axis_index("fsdp")
    core, chip = lax.rem(f, 2), f // 2
    other = 1 - core
    enc = sec < n_sec // 2
    even, odd = core == 0, core == 1
    dec = jnp.logical_not(enc)
    partner = {"fsdp": chip * 2 + other}
    nxt = {"section": lax.rem(sec + 1, n_sec)}
    prv = {"section": lax.rem(sec + n_sec - 1, n_sec)}

    def ahead(k):
        return lax.rem(chip + k, chips)

    def behind(k):
        return lax.rem(chip + chips - k, chips)

    def peer(h):
        return {"fsdp": h * 2 + core}

    def remote(src, dst, send, recv, dev):
        return pltpu.make_async_remote_copy(
            src_ref=src, dst_ref=dst, send_sem=send, recv_sem=recv,
            device_id=dev, device_id_type=pl.DeviceIdType.MESH,
        )

    def at(start, size):
        return pl.ds(pl.multiple_of(start, 16), size)

    def cols(j):
        return pl.ds(j * cn, cn)

    def fine(j):
        b, c = cuts[j]
        return pl.ds(b * cn + c * (cn // CUTS[b]), cn // CUTS[b])

    barrier = pltpu.get_barrier_semaphore()
    greet = [partner, prv] + [peer(ahead(k)) for k in range(1, chips)]
    with jax.named_scope("signal"):
        for dev in greet:
            pl.semaphore_signal(barrier, inc=1, device_id=dev, device_id_type=pl.DeviceIdType.MESH)

    x_rows, y_rows = chunk_of(rows), chunk_of(t_rows)
    gain_copy = pltpu.make_async_copy(gain_hbm, gain_ref, load.at[4])
    len_copy = pltpu.make_async_copy(len_hbm, len_ref, load.at[5])
    y_copy = pltpu.make_async_copy(y_hbm, yin, load.at[6])
    w_copies = [pltpu.make_async_copy(w_hbm.at[0, i], w.at[i], load.at[i]) for i in range(4)]
    x_copies = [
        pltpu.make_async_copy(
            x_hbm.at[pl.ds(r * x_rows, x_rows)], xin.at[pl.ds(r * x_rows, x_rows)], load.at[7 + r]
        )
        for r in range(rows // x_rows)
    ]
    gain_copy.start()
    for cp in x_copies:
        cp.start()
    y_copy.start()
    gain_copy.wait()
    gain = gain_ref[...]

    def arrived(r):
        x_copies[r].wait()
        if r == len(x_copies) - 1:
            for cp in w_copies:
                cp.start()
            len_copy.start()

    def block(h, which):
        return at((h * 2 + which) * rows, rows)

    def entered():
        pl.semaphore_wait(barrier, len(greet))

    kept = n_g - MOVED

    def send_rows(r):
        some = at(f * rows + r * x_rows, x_rows)
        for k in range(1, chips):
            spot = xs.at[some, pl.ds(*spans[0])]
            remote(spot, spot, ag_s.at[k - 1], ag_r.at[k - 1, 0], peer(ahead(k))).start()

    @pl.when(enc)
    def _():
        for r in range(len(x_copies)):
            arrived(r)
            xs[at(f * rows + r * x_rows, x_rows), :] = rms_norm(
                xin[pl.ds(r * x_rows, x_rows), :], gain
            )
            if r == 0:
                entered()
            send_rows(r)

    @pl.when(dec)
    def _():
        for r in range(len(x_copies)):
            arrived(r)
        xs[at(f * rows, rows), :] = xin[...]
        entered()
        for r in range(len(x_copies)):
            send_rows(r)

    def gather_send(k, j):
        spot = xs.at[block(chip, core), pl.ds(*spans[j])]
        return remote(spot, spot, ag_s.at[k - 1], ag_r.at[k - 1, j], peer(ahead(k)))

    def gather_recv(k, j):
        spot = xs.at[block(behind(k), core), pl.ds(*spans[j])]
        return remote(spot, spot, ag_s.at[k - 1], ag_r.at[k - 1, j], peer(behind(k)))

    def forward(k, j, which):
        spot = xs.at[block(behind(k), which), pl.ds(*spans[j])]
        return remote(spot, spot, fw_s.at[k - 1], fw_r.at[k - 1, j], partner)

    def moved_send(k, j):
        spot = xs.at[at(chip * pair, pair), pl.ds(*spans[j])]
        return remote(spot, spot, mv_s.at[0], ag_r.at[k - 1, j], peer(ahead(k)))

    def moved_recv(k, j):
        spot = xs.at[at(behind(k) * pair, pair), pl.ds(*spans[j])]
        return remote(spot, spot, mv_s.at[0], ag_r.at[k - 1, j], peer(behind(k)))

    def moved_forward(k, j):
        spot = xs.at[at(behind(k) * pair, pair), pl.ds(*spans[j])]
        return remote(spot, spot, mv_s.at[1], fw_r.at[k - 1, j], partner)

    def swap(which):
        spot = xs.at[block(chip, which), :]
        return remote(spot, spot, pt_s, pt_r, partner)

    for j in range(1, kept):
        for k in range(1, chips):
            gather_send(k, j).start()
    swap(core).start()

    def shift_source(j, src):
        return remote(src.at[:, fine(j)], so.at[:, fine(j)], ss_s, ss_r, nxt)

    def half(which):
        return at(which * t_half, t_half)

    def shift_target(j, src):
        return remote(src, to.at[half(core), cols(j)], ts_s, ts_r.at[j // (n_p // 2)], nxt)

    with jax.named_scope("y_wait"):
        y_copy.wait()

    @pl.when(enc)
    def _():
        for j in range(n_p):
            shift_target(j, yin.at[half(core), cols(j)]).start()

    @pl.when(dec)
    def _():
        for j in range(len(cuts)):
            shift_source(j, xin).start()

    scales = (HEAD_DIM**-0.5 * math.log2(math.e), None, None)

    def store(which, start, count, value):
        if scales[which] is not None:
            value = value * scales[which]
        qkv[which, at(start, count), :] = value.astype(BF16)

    def project(src, which, start, count):
        store(which, start, count, jnp.dot(src, w[which], preferred_element_type=F32))

    def project_piece(which, h, group):
        lanes = pl.ds(spans[group[0]][0], sum(spans[j][1] for j in group))
        part = jnp.dot(
            xs[at(h * pair, pair), lanes], w[which, lanes, :], preferred_element_type=F32
        )
        if group[0]:
            part = part + acc[which]
        if group[-1] < n_g - 1:
            acc[which] = part
        else:
            store(which, h * pair, pair, part)

    @pl.when(dec)
    def _():
        def step(r, carry):
            spot = at(r * y_rows, y_rows)
            ny[spot, :] = rms_norm(yin[spot, :], gain)
            return carry

        lax.fori_loop(0, t_rows // y_rows, step, 0)

    with jax.named_scope("wait_w0"):
        w_copies[0].wait()

    @pl.when(dec)
    def _():
        with jax.named_scope("proj_ny"):
            project(ny[...], 0, 0, t_rows)

    with jax.named_scope("wait_swap"):
        swap(other).wait_recv()

    @pl.when(odd)
    def _():
        for j in range(kept, n_g):
            for k in range(1, chips):
                moved_send(k, j).start()

    @pl.when(enc)
    def _():
        with jax.named_scope("proj_q"):
            project(xs[at(chip * pair, pair), :], 0, chip * pair, pair)

    for which in (1, 2):
        with jax.named_scope(f"wait_w{which}"):
            w_copies[which].wait()
        with jax.named_scope(f"proj_{which}"):
            project(xs[at(chip * pair, pair), :], which, chip * pair, pair)

    w_copies[3].wait()

    def flip(blocks):
        with jax.named_scope("flip"):
            for j in blocks:
                wt[:, cols(j)] = w[3, cols(j), :].T

    def consume(k, *group):
        for j in group:
            with jax.named_scope(f"fwait{j}"):
                if j < kept:
                    forward(k, j, other).wait_recv()
                else:
                    @pl.when(even)
                    def _():
                        moved_forward(k, j).wait_recv()

        @pl.when(enc)
        def _():
            with jax.named_scope(f"pp0_{j}"):
                project_piece(0, behind(k), group)

        with jax.named_scope(f"pp12_{j}"):
            project_piece(1, behind(k), group)
            project_piece(2, behind(k), group)

    def receive(k, j):
        with jax.named_scope(f"gwait{j}"):
            if j < kept:
                gather_recv(k, j).wait_recv()
                forward(k, j, core).start()
            else:
                @pl.when(odd)
                def _():
                    moved_recv(k, j).wait_recv()
                    moved_forward(k, j).start()

    flip(range(n_p if chips == 1 else n_p // 2))
    for k in range(1, chips):
        for j in range(kept - 1):
            receive(k, j)
            if j:
                consume(k, j - 1)
            if k == 1 and 1 <= j <= 2:
                flip(range(n_p * (j + 1) // 4, n_p * (j + 2) // 4))
        receive(k, kept - 1)
        receive(k, kept)
        consume(k, kept - 2)
        for j in range(kept + 1, n_g):
            receive(k, j)
        consume(k, kept - 1, kept)
        for j in range(kept + 1, n_g):
            consume(k, j)

    with jax.named_scope("wait_len"):
        len_copy.wait()
    length = len_ref[0]

    def attend(start, count):
        sure = total // 2 // 128 * 128
        key_ok = sure + lax.broadcasted_iota(jnp.int32, (1, total - sure), 1) < length
        first = lax.broadcasted_iota(jnp.int32, (1, 2 * HEAD_DIM), 1) < HEAD_DIM
        ones = jnp.ones((total, 2 * HEAD_DIM), BF16)

        def score(t):
            lanes = pl.ds(t * 2 * HEAD_DIM, 2 * HEAD_DIM)
            queries = qkv[0, at(start, count), lanes]
            zero = jnp.zeros_like(queries)
            both = jnp.concatenate(
                [jnp.where(first, queries, zero), jnp.where(first, zero, queries)], axis=0
            )
            return lax.dot_general(
                both, qkv[1, :total, lanes], (((1,), (1,)), ((), ())), preferred_element_type=F32
            )

        def weigh(scores):
            tail = jnp.where(key_ok, scores[:, sure:], -1000000000.0 * math.log2(math.e))
            if sure:
                scores = jnp.concatenate([scores[:, :sure], tail], axis=1)
            else:
                scores = tail
            return jnp.exp2(scores - jnp.max(scores, axis=-1, keepdims=True)).astype(BF16)

        def mix(t, expo):
            lanes = pl.ds(t * 2 * HEAD_DIM, 2 * HEAD_DIM)
            values = jnp.concatenate([qkv[2, :total, lanes], ones], axis=1)
            mixed = jnp.dot(expo, values, preferred_element_type=F32)
            mixed = mixed[:, : 2 * HEAD_DIM] * (1.0 / mixed[:, 2 * HEAD_DIM :])
            ctx[at(start, count), lanes] = jnp.where(
                first, mixed[:count], mixed[count:]
            ).astype(BF16)

        with jax.named_scope("attend"):
            pairs = range(width // (2 * HEAD_DIM))
            scores = [score(t) for t in pairs]
            weights = [weigh(block) for block in scores]
            for t in pairs:
                mix(t, weights[t])

    def out_piece(start, count, dst, j):
        with jax.named_scope("outp"):
            dst[:, cols(j)] = jnp.dot(
                ctx[at(start, count), :], wt[:, cols(j)], preferred_element_type=F32
            ).astype(BF16)

    def mate_term(k, j):
        return remote(
            term.at[k - 1, at(other * rows, rows), cols(j)], prt.at[k - 1, :, cols(j)],
            t1_s.at[k - 1], fw_r.at[k - 1, j], partner,
        )

    def send_sum(k, j):
        return remote(
            sums.at[k - 1, :, fine(j)], rem.at[k - 1, :, fine(j)],
            x1_s.at[k - 1], x1_r.at[k - 1, j], peer(ahead(k)),
        )

    def mate_own(j):
        return remote(
            own.at[at(other * rows, rows), cols(j)], prt_own.at[:, cols(j)],
            t2_s, load.at[j], partner,
        )

    def mate_target(j):
        return remote(
            dterm.at[half(other), cols(j)], dprt.at[:, cols(j)], t1_s.at[0], fw_r.at[0, j], partner
        )

    def send_target(k, j):
        return remote(
            dp.at[chip, :, cols(j)], dp.at[chip, :, cols(j)],
            x1_s.at[k - 1], x1_r.at[k - 1, j], peer(ahead(k)),
        )

    def recv_target(k, j):
        spot = dp.at[behind(k), :, cols(j)]
        return remote(spot, spot, x1_s.at[k - 1], x1_r.at[k - 1, j], peer(behind(k)))

    @pl.when(enc)
    def _():
        def term_piece(k, j):
            out_piece(ahead(k) * pair, pair, term.at[k - 1], j)
            mate_term(k, j).start()

        def pass_on(k, j):
            with jax.named_scope("mtw"):
                mate_term(k, j).wait_recv()
            mine = term[k - 1, at(core * rows, rows), cols(j)].astype(F32)
            sums[k - 1, :, cols(j)] = (mine + prt[k - 1, :, cols(j)].astype(F32)).astype(BF16)
            for piece, (b, _) in enumerate(cuts):
                if b == j:
                    send_sum(k, piece).start()

        def own_piece(j):
            out_piece(chip * pair, pair, own, j)
            mate_own(j).start()

        def finish(j):
            if cuts[j][1] == 0:
                with jax.named_scope("mow"):
                    mate_own(cuts[j][0]).wait_recv()
            delta = own[at(core * rows, rows), fine(j)].astype(F32) + prt_own[:, fine(j)].astype(F32)
            for k in range(1, chips):
                with jax.named_scope(f"ssw{j}"):
                    send_sum(k, j).wait_recv()
                delta += rem[k - 1, :, fine(j)].astype(F32)
            fin[:, fine(j)] = (xin[:, fine(j)].astype(F32) + delta).astype(BF16)
            shift_source(j, fin).start()

        for k in range(1, chips - 1):
            attend(ahead(k) * pair, pair)
            for j in range(n_p):
                term_piece(k, j)
                if j:
                    pass_on(k, j - 1)
            pass_on(k, n_p - 1)

        last = chips - 1
        acts = {"O": lambda j: term_piece(last, j), "S": lambda j: pass_on(last, j),
                "W": own_piece, "F": finish}
        if last:
            for which in (other, core):
                start = ahead(last) * pair + which * rows
                attend(start, rows)
                out_piece(start, rows, term.at[last - 1, at(which * rows, rows)], 0)
                if which is other:
                    mate_term(last, 0).start()
            for name, j in LEAD:
                acts[name](j)
        for which in (other, core):
            start = chip * pair + which * rows
            attend(start, rows)
            out_piece(start, rows, own.at[at(which * rows, rows)], 0)
            if which is other:
                mate_own(0).start()
                if last:
                    pass_on(last, 1)
        for name, j in TRAIL:
            if last or name in "WF":
                acts[name](j)
        whole = pl.ds(0, rows)
        remote(own.at[whole], prt_own, t2_s, load.at[0], partner).wait_send()
        for k in range(1, chips):
            remote(
                term.at[k - 1, whole], prt.at[k - 1], t1_s.at[k - 1], fw_r.at[k - 1, 0], partner
            ).wait_send()
            remote(
                sums.at[k - 1], rem.at[k - 1], x1_s.at[k - 1], x1_r.at[k - 1, 0], peer(ahead(k))
            ).wait_send()

    @pl.when(dec)
    def _():
        attend(0, t_rows)

        def pass_on(j):
            with jax.named_scope("mtgw"):
                mate_target(j).wait_recv()
            mine = dterm[half(core), cols(j)].astype(F32)
            dp[chip, :, cols(j)] = (mine + dprt[:, cols(j)].astype(F32)).astype(BF16)
            for k in range(1, chips):
                send_target(k, j).start()

        for j in range(n_p):
            out_piece(0, t_rows, dterm, j)
            mate_target(j).start()
            if j > 2:
                pass_on(j - 3)
        for j in range(n_p - 3, n_p):
            pass_on(j)
        for j in range(n_p):
            for k in range(1, chips):
                with jax.named_scope(f"rtw{j}"):
                    recv_target(k, j).wait_recv()
            delta = dp[0, :, cols(j)].astype(F32)
            for h in range(1, chips):
                delta += dp[h, :, cols(j)].astype(F32)
            yfin[:, cols(j)] = (yin[half(core), cols(j)].astype(F32) + delta).astype(BF16)
            shift_target(j, yfin.at[:, cols(j)]).start()
        remote(dterm.at[half(other)], dprt, t1_s.at[0], fw_r.at[0, 0], partner).wait_send()
        for k in range(1, chips):
            remote(
                dp.at[chip], dp.at[chip], x1_s.at[k - 1], x1_r.at[k - 1, 0], peer(ahead(k))
            ).wait_send()

    def cross(which, lanes):
        spot = to.at[half(which), lanes]
        return remote(spot, spot, tf_s, tf_r, partner)

    for j in range(2):
        part = pl.ds(j * (d // 2), d // 2)
        with jax.named_scope(f"stw{j}"):
            remote(yfin.at[:, part], to.at[half(core), part], ts_s, ts_r.at[j], nxt).wait_recv()
        cross(core, part).start()
    every = pl.ds(0, d)
    shifted = remote(fin, so, ss_s, ss_r, nxt)
    with jax.named_scope("shw"):
        shifted.wait_recv()
    with jax.named_scope("crw"):
        cross(other, every).wait_recv()

    with jax.named_scope("end"):
        swap(core).wait_send()
        for k in range(1, chips):
            sent = pl.ds(0, spans[kept][0])
            mine, theirs = xs.at[block(chip, core), sent], xs.at[block(behind(k), core), sent]
            remote(mine, mine, ag_s.at[k - 1], ag_r.at[k - 1, 0], peer(ahead(k))).wait_send()
            remote(theirs, theirs, fw_s.at[k - 1], fw_r.at[k - 1, 0], partner).wait_send()
        if chips > 1:
            late = pl.ds(0, d - spans[kept][0])

            @pl.when(odd)
            def _():
                for way, dev in ((0, peer(ahead(1))), (1, partner)):
                    spot = xs.at[pl.ds(0, total - pair), late]
                    remote(spot, spot, mv_s.at[way], fw_r.at[0, 0], dev).wait_send()

        shifted.wait_send()
        remote(yfin, to.at[half(core)], ts_s, ts_r.at[0], nxt).wait_send()
        cross(core, every).wait_send()


def local(n_sec, n_f, source_rows, target_rows, attn_weights, gains, lengths):
    chips = n_f // 2
    more = max(chips - 1, 1)
    rows, d = source_rows.shape
    t_rows = target_rows.shape[0]
    width = attn_weights.shape[3]
    pair, total, t_half = 2 * rows, rows * n_f, t_rows // 2
    q_rows = max(total, t_rows)
    n_g, n_p = len(GATHER), BLOCKS
    dma = pltpu.SemaphoreType.DMA
    vmem = lambda *shape: pltpu.VMEM(shape, BF16)
    scratch = [
        vmem(rows, d), vmem(t_rows, d), pltpu.VMEM((1, d), F32), pltpu.SMEM((1,), jnp.int32),
        vmem(total, d), vmem(t_rows, d), vmem(4, d, width), vmem(width, d), pltpu.VMEM((3, pair, width), F32),
        vmem(3, q_rows, width), vmem(q_rows, width),
        vmem(more, pair, d), vmem(more, rows, d), vmem(more, rows, d), vmem(more, rows, d),
        vmem(pair, d), vmem(rows, d), vmem(rows, d),
        vmem(t_rows, d), vmem(t_half, d), vmem(chips, t_half, d), vmem(t_half, d),
        dma((max(7 + rows // chunk_of(rows), n_p),)),
        dma((more,)), dma((more, n_g)), dma, dma, dma((more,)), dma((more, max(n_g, n_p))), dma((2,)),
        dma((more,)), dma((more,)), dma((more, sum(CUTS))), dma,
        dma, dma, dma, dma((2,)), dma, dma,
    ]
    anywhere = pl.BlockSpec(memory_space=pl.ANY)
    moved = pl.pallas_call(
        functools.partial(kernel, n_sec, n_f),
        out_shape=(
            pltpu.VMEM(source_rows.shape, BF16),
            pltpu.VMEM(target_rows.shape, BF16),
        ),
        in_specs=[anywhere] * 5,
        out_specs=(anywhere, anywhere),
        scratch_shapes=scratch,
        compiler_params=pltpu.CompilerParams(
            collective_id=0, has_side_effects=True, vmem_limit_bytes=56 * 1024 * 1024
        ),
    )(source_rows, target_rows, gains, lengths, attn_weights)
    return settle(*moved)


def settle(source, target):
    def body(a_ref, b_ref, a_out, b_out, sem):
        plan = []
        for src, dst in ((a_ref, a_out), (b_ref, b_out)):
            step = src.shape[0] // 2
            for j in range(2):
                some = pl.ds(j * step, step)
                plan.append(pltpu.make_async_copy(src.at[some], dst.at[some], sem.at[len(plan)]))
        for copy in plan:
            copy.start()
        for copy in plan:
            copy.wait()

    anywhere = pl.BlockSpec(memory_space=pl.ANY)
    return pl.pallas_call(
        body,
        out_shape=tuple(jax.ShapeDtypeStruct(v.shape, v.dtype) for v in (source, target)),
        in_specs=[anywhere, anywhere],
        out_specs=(anywhere, anywhere),
        scratch_shapes=[pltpu.SemaphoreType.DMA((4,))],
        compiler_params=pltpu.CompilerParams(vmem_limit_bytes=8 * 1024 * 1024),
    )(source, target)


def solution(mesh):
    in_specs = (
        P(("section", "fsdp"), None),
        P("section", None),
        P("section", None, None, "fsdp"),
        P("section", None),
        P("section"),
    )
    out_specs = (P(("section", "fsdp"), None), P("section", None))
    body = functools.partial(local, mesh.shape["section"], mesh.shape["fsdp"])
    return jax.shard_map(body, mesh=mesh, in_specs=in_specs, out_specs=out_specs, check_vma=False)
```
